32 devices in a mesh: row: 8 (over z, core), col: 4 (over y, x).
Axes of the slice: x: 2, y: 2, z: 4, core: 2. Of those that a mesh axis runs over, the one named last changes fastest.
Arguments:
- act_codes: int32 [512, 7168], P('col', 'row'), may hold values from -127 to 127
- act_scales: float32 [512, 112], P('col', 'row'), may hold values from 0.005 to 0.03
- gate_weight: bfloat16 [7168, 18432], P('row', 'col'), may hold values from -0.0625 to 0.0625
- up_weight: bfloat16 [7168, 18432], P('row', 'col'), may hold values from -0.0625 to 0.0625
- down_weight: bfloat16 [18432, 7168], P('col', 'row'), may hold values from -0.046875 to 0.046875
Outputs:
- mixed: bfloat16 [512, 7168], P('col', 'row')
The draws below stay inside these ranges and needn't reach their ends.
All inputs are finite; a program needn't handle non-finite values.
Results may differ from the reference program's by a relative error of at most 0.03.
Values may be sent and summed in bfloat16 or wider, within the bound.
No kernel may reach another device: no remote copies, remote signals or barrier semaphores. Data moves between devices by JAX's collectives and lax.ppermute only.
A program may use at most 128 MiB of HBM per device.

```python
import math
import jax
import jax.numpy as jnp
from jax import lax

D = 7168
FF = 18432
QB = 64
TOKENS = 512
D_ROW = 896
FF_COL = 4608
BLOCKS = 112
N_ROW = 8
N_COL = 4


def place_ends(entries, rng, least, top_value):
    index_at = [jax.random.randint(jax.random.fold_in(rng, axis), (), 0, length) for axis, length in enumerate(entries.shape)]
    widest = entries.shape.index(max(entries.shape))
    next_to = index_at[:widest] + [(index_at[widest] + 1) % entries.shape[widest]] + index_at[widest + 1:]
    return entries.at[tuple(index_at)].set(least).at[tuple(next_to)].set(top_value)


def shard_levels(own_key, dims, cuts, smallest, high):
    loudness, own = 1.0, jax.random.fold_in(own_key, 6)
    for axis_at, blocks in cuts:
        steps = jnp.exp(jax.random.uniform(jax.random.fold_in(own, axis_at), (blocks,), jnp.float32, smallest / len(cuts), high / len(cuts)))
        loudness = loudness * jnp.repeat(steps, dims[axis_at] // blocks).reshape([-1 if axis == axis_at else 1 for axis in range(len(dims))])
    return loudness


def centred(key, extent, width, most, cuts=(), kind=jnp.bfloat16):
    values = jax.random.normal(key, extent, jnp.float32) * width
    if len(cuts) > 0:
        values = shard_levels(key, extent, cuts, -0.22, 0.18) * values
    return jnp.clip(values, min=-most, max=most).astype(kind)


def setup_inputs(seed: int = 0) -> dict:
    keys = jax.random.split(jax.random.key(seed), 6)
    act_codes = place_ends(jax.random.randint(keys[0], (TOKENS, D), -127, 128), jax.random.fold_in(keys[0], 1), -127, 127).astype(jnp.int32)
    act_scales = jnp.clip(jnp.exp(math.log(0.03) - 1.7917595 * jax.random.uniform(keys[1], (TOKENS, BLOCKS), jnp.float32) ** shard_levels(keys[1], (TOKENS, BLOCKS), ((0, 4), (1, 8)), -0.2, 0.2)), 0.005, 0.03)
    gate_weight = centred(keys[2], (D, FF), D ** -0.5, 0.0625, ((0, 8), (1, 4)))
    up_weight = centred(keys[3], (D, FF), D ** -0.5, 0.0625, ((0, 8), (1, 4)))
    down_weight = centred(keys[4], (FF, D), FF ** -0.5, 0.046875, ((0, 4), (1, 8)))
    return dict(act_codes=act_codes, act_scales=act_scales, gate_weight=gate_weight, up_weight=up_weight, down_weight=down_weight)


def dequantize(act_codes, act_scales):
    rows = act_codes.shape[0]
    blocked = act_codes.astype(jnp.float32).reshape(rows, BLOCKS, QB)
    scaled = blocked * act_scales[:, :, None]
    return scaled.reshape(rows, D).astype(jnp.bfloat16)


def rounded(value):
    narrow = lax.optimization_barrier(value.astype(jnp.bfloat16))
    return narrow.astype(jnp.float32)


def reference(act_codes, act_scales, gate_weight, up_weight, down_weight):
    acts = dequantize(act_codes, act_scales)

    def feature_group(index, totals):
        start = (index * D_ROW).astype(jnp.int32)
        slab = lax.dynamic_slice_in_dim(acts, start, D_ROW, 1)
        gate_rows = lax.dynamic_slice_in_dim(gate_weight, start, D_ROW, 0)
        up_rows = lax.dynamic_slice_in_dim(up_weight, start, D_ROW, 0)
        gate_part = rounded(jnp.dot(slab, gate_rows, preferred_element_type=jnp.float32))
        up_part = rounded(jnp.dot(slab, up_rows, preferred_element_type=jnp.float32))
        return (totals[0] + gate_part, totals[1] + up_part)

    empty = jnp.zeros((TOKENS, FF), jnp.float32)
    gate, up = lax.fori_loop(0, N_ROW, feature_group, (empty, empty))
    hidden = (jax.nn.silu(gate) * up).astype(jnp.bfloat16)

    def hidden_group(index, total):
        start = (index * FF_COL).astype(jnp.int32)
        slab = lax.dynamic_slice_in_dim(hidden, start, FF_COL, 1)
        rows_down = lax.dynamic_slice_in_dim(down_weight, start, FF_COL, 0)
        return total + rounded(jnp.dot(slab, rows_down, preferred_element_type=jnp.float32))

    mixed = lax.fori_loop(0, N_COL, hidden_group, jnp.zeros((TOKENS, D), jnp.float32))
    return mixed.astype(jnp.bfloat16)
```

```python
import jax
import jax.numpy as jnp
from jax import lax
from jax.sharding import PartitionSpec as P


STREAMS = (4, 3, 1)
F32, BF16 = jnp.float32, jnp.bfloat16


def add(a, b):
    return a.astype(F32) + b.astype(F32)


def on_device(n_row, n_col, streams, act_codes, act_scales, gate_weight, up_weight, down_weight):
    tokens, width = act_codes.shape
    nblocks = act_scales.shape[1]
    chips = n_row // 2
    mid = chips // 2
    hidden_width = gate_weight.shape[1] // streams
    row, col = lax.axis_index("row"), lax.axis_index("col")
    z = row // 2
    q = 2 * (z >= mid).astype(jnp.int32) + row % 2
    per_group = n_col // 4
    swap = [(i, i ^ 1) for i in range(n_row)]

    def hop(h):
        pairs = [(h, h + 1), (chips - 1 - h, chips - 2 - h)]
        return [(2 * a + c, 2 * b + c) for a, b in pairs for c in range(2)]

    blocked = act_codes.astype(F32).reshape(tokens, nblocks, width // nblocks)
    acts = (blocked * act_scales[:, :, None]).reshape(tokens, width).astype(BF16)
    every = lax.all_gather(acts, "col", axis=0, tiled=False)

    groups = every.reshape(4, per_group * tokens, width)
    x = jnp.concatenate([lax.dynamic_index_in_dim(groups, q ^ k, 0, False) for k in (3, 1, 2, 0)])

    def front(s):
        part = slice(s * hidden_width, (s + 1) * hidden_width)
        sides = [jnp.dot(x, w[:, part], preferred_element_type=F32).astype(BF16)
                 for w in (gate_weight, up_weight)]
        half = x.shape[0] // 2
        other = jnp.concatenate([v[:half] for v in sides], axis=1)
        mine = jnp.concatenate([v[half:] for v in sides], axis=1)
        return s, mine, lax.ppermute(other, "row", swap)

    def middle(s, mine, received):
        rows = mine.shape[0] // 2
        both = add(mine, received).astype(BF16)
        far, near = both[:rows], both[rows:]
        for h in range(chips - 1):
            got = lax.ppermute(far if h < mid else near, "row", hop(h))
            if h + 1 < mid:
                far = add(far, got).astype(BF16)
            else:
                near = add(near, got)
                if h < chips - 2:
                    near = near.astype(BF16)
        hidden = (jax.nn.silu(near[:, :hidden_width]) * near[:, hidden_width:]).astype(BF16)
        h_near, h_far = hidden, None
        for k in range(chips - 1):
            got = lax.ppermute(h_near if k < mid else h_far, "row", hop(k))
            here = (z == k + 1) | (z == chips - 2 - k)
            if k + 1 < mid:
                h_near = jnp.where(here, got, h_near)
            else:
                h_far = got if h_far is None else jnp.where(here, got, h_far)
        both = jnp.concatenate([h_near, h_far])
        full = jnp.concatenate([both, lax.ppermute(both, "row", swap)])
        rows_down = down_weight[s * hidden_width:(s + 1) * hidden_width]
        return jnp.dot(full, rows_down, preferred_element_type=F32)

    def back(y):
        y = y.reshape(n_col, tokens, y.shape[1])

        def block(dest):
            g = (dest // per_group) ^ q
            at = (g % 2) * 2 + g // 2
            return lax.dynamic_index_in_dim(y, at * per_group + dest % per_group, 0, False)

        total = block(col)
        for k in list(range(n_col - 1, 0, -1)):
            if n_col & (n_col - 1) == 0:
                dest, pairs = col ^ k, [(c, c ^ k) for c in range(n_col)]
            else:
                dest, pairs = (col + k) % n_col, [(c, (c + k) % n_col) for c in range(n_col)]
            total = total + lax.ppermute(block(dest).astype(BF16), "col", pairs).astype(F32)
        return total.astype(BF16)

    fronts = [front(s) for s in range(streams)]
    return back(sum(middle(*f) for f in fronts))


def streams_of(width):
    return next(s for s in STREAMS if width % (s * 128) == 0 or s == 1)


def solution(mesh):
    placed = (P("col", "row"), P("col", "row"), P("row", "col"), P("row", "col"), P("col", "row"))
    n_row, n_col = mesh.shape["row"], mesh.shape["col"]

    def body(*args):
        return on_device(n_row, n_col, streams_of(args[2].shape[1]), *args)

    return jax.shard_map(body, mesh=mesh, in_specs=placed, out_specs=P("col", "row"), check_vma=False)
```
